32 devices in a mesh: seq: 8 (over y, x, core), head: 4 (over z).
Axes of the slice: x: 2, y: 2, z: 4, core: 2. Of those that a mesh axis runs over, the one named last changes fastest.
Arguments:
- queries: bfloat16 [8192, 2048], P('seq', 'head'), may hold values from -6 to 6
- keys: bfloat16 [8192, 2048], P('seq', 'head'), may hold values from -100 to 100
- values: bfloat16 [8192, 2048], P('seq', 'head'), may hold values from -16 to 16
- gates: float32 [8192, 16], P('seq', 'head'), may hold values from 0.05 to 1
- ridge: float32 [16], P('head'), may hold values from 0.25 to 4
- out_weight: bfloat16 [2048, 2048], P(None, 'head'), may hold values from -0.125 to 0.125
Outputs:
- partial_out: bfloat16 [4, 8192, 2048], P('head', 'seq')
The draws below stay inside these ranges and needn't reach their ends.
All inputs are finite; a program needn't handle non-finite values.
Results may differ from the reference program's by a relative error of at most 0.0049.
Values may be sent and summed in bfloat16 or wider, within the bound.
A program may use at most 128 MiB of HBM per device.

```python
import math
import jax
import jax.numpy as jnp
from jax import lax

D = 2048
HEADS = 16
HD = 128
SPAN = 128
ITERS = 8
TOKENS = 8192
N_HEAD = 4


def key_value_pair(key):
    scale_key = jax.random.fold_in(key, 101)
    normal_key = jax.random.fold_in(key, 202)
    mixing_key = jax.random.fold_in(key, 303)
    noise_key = jax.random.fold_in(key, 404)
    columns = HEADS * HD
    spread = math.log(10.0)
    scales = jnp.exp(jax.random.uniform(scale_key, (columns,), jnp.float32, 0.0, spread))
    base = jax.random.normal(normal_key, (TOKENS, columns), jnp.float32)
    raw_keys = jnp.clip(base * scales, -100.0, 100.0)
    grouped = raw_keys.reshape(TOKENS, HEADS, HD)
    unit_keys = grouped * lax.rsqrt(jnp.sum(grouped * grouped, -1, keepdims=True) + 1e-06)
    mixing = jax.random.normal(mixing_key, (HEADS, HD, HD), jnp.float32)
    mapped = jnp.einsum('thd,hde->the', unit_keys, mixing)
    noisy = mapped + 0.7 * jax.random.normal(noise_key, (TOKENS, HEADS, HD), jnp.float32)
    return (raw_keys, jnp.clip(noisy, -16.0, 16.0).reshape(TOKENS, columns))


def draw_keys(key, part):
    return key_value_pair(key)[0].astype(jnp.bfloat16)


def draw_values(key, part):
    return key_value_pair(key)[1].astype(jnp.bfloat16)


def block_scale(rng, shape, pieces, least, high):
    gain, own = 1.0, jax.random.fold_in(rng, 6)
    for axis_at, shards_of in pieces:
        heights = jnp.exp(jax.random.uniform(jax.random.fold_in(own, axis_at), (shards_of,), jnp.float32, least / len(pieces), high / len(pieces)))
        gain = gain * jnp.repeat(heights, shape[axis_at] // shards_of).reshape([-1 if axis == axis_at else 1 for axis in range(len(shape))])
    return gain


def normal_values(key, shape, deviation, bound, cuts=(), held_as=jnp.bfloat16):
    factor_of = block_scale(key, shape, cuts, -0.22, 0.18) if cuts else 1.0
    result = jax.random.normal(key, shape, jnp.float32) * deviation * factor_of
    return jnp.minimum(jnp.maximum(result, -bound), bound).astype(held_as)


def setup_inputs(seed: int = 0) -> dict:
    streams_of = jax.random.split(jax.random.key(seed), 7)
    return {
        "queries": normal_values(streams_of[0], (TOKENS, HEADS * HD), 1.0, 6.0, ((0, 8), (1, 4))),
        "keys": draw_keys(jax.random.fold_in(streams_of[6], 71), 0),
        "values": draw_values(jax.random.fold_in(streams_of[6], 71), 0),
        "gates": jnp.clip(jnp.exp(math.log(1.0) - 2.9957323 * jax.random.uniform(streams_of[3], (TOKENS, HEADS), jnp.float32) ** block_scale(streams_of[3], (TOKENS, HEADS), ((0, 8), (1, 4)), -0.2, 0.2)), 0.05, 1.0),
        "ridge": jnp.clip(jnp.exp(math.log(4.0) - 2.7725887 * jax.random.uniform(streams_of[4], (HEADS,), jnp.float32) ** block_scale(streams_of[4], (HEADS,), ((0, 4),), -0.2, 0.2)), 0.25, 4.0),
        "out_weight": normal_values(streams_of[5], (HEADS * HD, D), (HEADS * HD) ** -0.5, 0.125, ((1, 4),)),
    }


highest = lax.Precision.HIGHEST

def unit_rows(matrix):
    return matrix * lax.rsqrt(lax.optimization_barrier(jnp.sum(matrix * matrix, -1, keepdims=True)) + 1e-06)

def solve_block(prior_gram, prior_moment, keys_unit, keys_gated, values_gated, queries_unit, ridge_column, causal_mask):

    def apply_system(direction):
        from_prior = jnp.einsum('...de,...te->...td', prior_gram, direction, precision=highest)
        correlations = jnp.einsum('...id,...td->...ti', keys_unit, direction, precision=highest) * causal_mask
        from_block = jnp.einsum('...ti,...id->...td', correlations, keys_gated, precision=highest)
        return from_prior + from_block + ridge_column * direction

    def sweep_once(sweep, state):
        solution, residual, direction, norm_now = state
        image = apply_system(direction)
        step_size = norm_now / (lax.optimization_barrier(jnp.sum(direction * image, -1, keepdims=True)) + 1e-06)
        solution = solution + step_size * direction
        residual = residual - step_size * image
        norm_next = lax.optimization_barrier(jnp.sum(residual * residual, -1, keepdims=True))
        direction = residual + norm_next / (norm_now + 1e-06) * direction
        return (solution, residual, direction, norm_next)
    start_state = (jnp.zeros_like(queries_unit), queries_unit, queries_unit, lax.optimization_barrier(jnp.sum(queries_unit * queries_unit, -1, keepdims=True)))
    solution = lax.fori_loop(0, ITERS, sweep_once, start_state)[0]
    correlations = jnp.einsum('...id,...td->...ti', keys_unit, solution, precision=highest) * causal_mask
    readout = jnp.einsum('...ed,...td->...te', prior_moment, solution, precision=highest)
    return readout + jnp.einsum('...ti,...ie->...te', correlations, values_gated, precision=highest)

def reference(queries, keys, values, gates, ridge, out_weight):
    blocks = TOKENS // SPAN

    def split(matrix):
        return matrix.astype(jnp.float32).reshape(blocks, SPAN, HEADS, HD).transpose(0, 2, 1, 3)
    queries_unit = unit_rows(split(queries))
    keys_unit = unit_rows(split(keys))
    gate_cols = gates.astype(jnp.float32).reshape(blocks, SPAN, HEADS).transpose(0, 2, 1)[..., None]
    keys_gated = keys_unit * gate_cols
    values_gated = split(values) * gate_cols
    positions = jnp.arange(SPAN)
    causal_mask = (positions[None, :] <= positions[:, None]).astype(jnp.float32)
    ridge_column = ridge.astype(jnp.float32)[:, None, None]

    def advance(carry, block):
        prior_gram, prior_moment = carry
        unit_block, gated_block, value_block, query_block = block
        readout = solve_block(prior_gram, prior_moment, unit_block, gated_block, value_block, query_block, ridge_column, causal_mask)
        prior_gram = prior_gram + jnp.einsum('hid,hie->hde', gated_block, unit_block, precision=highest)
        prior_moment = prior_moment + jnp.einsum('hie,hid->hed', value_block, unit_block, precision=highest)
        return ((prior_gram, prior_moment), readout)
    zeros = jnp.zeros((HEADS, HD, HD), jnp.float32)
    _, readouts = lax.scan(advance, (zeros, zeros), (keys_unit, keys_gated, values_gated, queries_unit))
    readout = readouts.transpose(0, 2, 1, 3).reshape(TOKENS, HEADS * HD).astype(jnp.bfloat16)
    group_width = HEADS * HD // N_HEAD
    slabs = []
    for group in range(N_HEAD):
        lower = group * group_width
        slabs.append(jnp.dot(readout[:, lower:lower + group_width], out_weight[lower:lower + group_width], preferred_element_type=jnp.float32))
    return jnp.stack(slabs).astype(jnp.bfloat16)
```

```python
import functools

import jax
import jax.numpy as jnp
from jax import lax
from jax.experimental import pallas as pl
from jax.experimental.pallas import tpu as pltpu
from jax.sharding import PartitionSpec as P

HD = 128
SPAN = 128
ITERS = 8
EPS = 1e-06
f32 = jnp.float32
bf16 = jnp.bfloat16
VMEM_BYTES = 56 * 1024 * 1024


def dot(a, b):
    return jnp.dot(a, b, preferred_element_type=f32)


def two_terms(x):
    high = x.astype(bf16)
    return high, (x - high.astype(f32)).astype(bf16)


def inverse_norm(columns):
    return lax.rsqrt(jnp.sum(columns * columns, 0, keepdims=True) + EPS)


def block_sums(keys, values, gate_row):
    keys_t = keys.astype(f32).T
    s = inverse_norm(keys_t)
    w_value = gate_row * s
    w_key = w_value * s
    gram = dot(
        jnp.concatenate(two_terms(keys_t * w_key), 1), jnp.concatenate([keys, keys], 0)
    )
    moment = dot(
        jnp.concatenate(two_terms(keys_t * w_value), 1), jnp.concatenate([values, values], 0)
    )
    return gram, moment, keys_t, w_key, w_value


def totals_kernel(k_ref, v_ref, g_ref, out_ref):
    gram = jnp.zeros((HD, HD), f32)
    moment = jnp.zeros((HD, HD), f32)
    for c in range(k_ref.shape[0] // SPAN):
        rows = pl.ds(c * SPAN, SPAN)
        block_gram, block_moment, *_ = block_sums(k_ref[rows], v_ref[rows], g_ref[:, rows])
        gram += block_gram
        moment += block_moment
    out_ref[0, 0] = gram
    out_ref[1, 0] = moment


def solve_kernel(
    q_ref, k_ref, v_ref, g_ref, ridge_ref, table_ref, out_ref,
    system, weights, weights_value, moments, sol, res, direct,
):
    h = pl.program_id(0)
    me = lax.axis_index("seq")
    blocks = k_ref.shape[0] // SPAN
    row = lax.broadcasted_iota(jnp.int32, (HD, HD), 0)
    col = lax.broadcasted_iota(jnp.int32, (HD, HD), 1)
    causal = row <= col
    gram = jnp.where(row == col, ridge_ref[h], 0.0)
    moment = jnp.zeros((HD, HD), f32)
    for n in range(table_ref.shape[0]):
        lower = jnp.where(n < me, 1.0, 0.0).astype(f32)
        gram += lower * table_ref[n, 0, 0]
        moment += lower * table_ref[n, 1, 0]
    start = []
    for c in range(blocks):
        rows = pl.ds(c * SPAN, SPAN)
        block_gram, block_moment, keys_t, w_key, w_value = block_sums(
            k_ref[rows], v_ref[rows], g_ref[:, rows]
        )
        high, low = two_terms(gram)
        system[c] = jnp.concatenate([high, high, low, keys_t.astype(bf16)], 1)
        weights[c] = jnp.where(causal, jnp.broadcast_to(w_key, (SPAN, SPAN)).T, 0.0)
        weights_value[c] = jnp.where(causal, jnp.broadcast_to(w_value, (SPAN, SPAN)).T, 0.0)
        high, low = two_terms(moment)
        moments[c] = jnp.concatenate([high, high, low], 0)
        gram += block_gram
        moment += block_moment
        queries = q_ref[rows].astype(f32).T
        queries = queries * inverse_norm(queries)
        sol[c] = jnp.zeros((HD, SPAN), f32)
        res[c] = queries
        direct[c] = queries
        start.append(jnp.sum(queries * queries, 0, keepdims=True))

    def sweep(_, norms):
        after = []
        for c in range(blocks):
            rows = pl.ds(c * SPAN, SPAN)
            keys = k_ref[rows]
            d = direct[c]
            high, low = two_terms(d)
            corr = dot(jnp.concatenate([keys, keys], 1), jnp.concatenate([high, low], 0))
            corr = (corr * weights[c]).astype(bf16)
            image = dot(system[c], jnp.concatenate([high, low, high, corr], 0))
            now = norms[c]
            step = now / (jnp.sum(d * image, 0, keepdims=True) + EPS)
            sol[c] = sol[c] + step * d
            r = res[c] - step * image
            res[c] = r
            following = jnp.sum(r * r, 0, keepdims=True)
            direct[c] = r + following / (now + EPS) * d
            after.append(following)
        return tuple(after)

    lax.fori_loop(0, ITERS, sweep, tuple(start))
    for c in range(blocks):
        rows = pl.ds(c * SPAN, SPAN)
        keys = k_ref[rows]
        values = v_ref[rows]
        high, low = two_terms(sol[c])
        corr = dot(jnp.concatenate([keys, keys], 1), jnp.concatenate([high, low], 0))
        corr_high, corr_low = two_terms(corr * weights_value[c])
        left = jnp.concatenate([high, low, high, corr_high, corr_low], 0)
        right = jnp.concatenate([moments[c], values, values], 0)
        out_ref[rows] = lax.dot_general(
            left, right, (((0,), (0,)), ((), ())), preferred_element_type=f32
        ).astype(out_ref.dtype)


def project_kernel(r_ref, *refs):
    *pieces, out_ref = refs
    count = len(pieces)
    me = lax.axis_index("head")
    readout = r_ref[...]
    for shift, piece in enumerate(pieces):
        width = piece.shape[1]
        owner = lax.rem(me + count - shift, count)
        columns = pl.ds(pl.multiple_of(owner * width, width), width)
        out_ref[0, :, columns] = dot(readout, piece[...]).astype(out_ref.dtype)


def shards(n_seq, n_head, queries, keys, values, gates, ridge, out_weight):
    tokens, head_width = queries.shape
    heads = head_width // HD
    blocks = tokens // SPAN
    me = lax.axis_index("head")

    def rows_of(device):
        return lax.dynamic_slice_in_dim(out_weight, device * head_width, head_width, 0)

    pieces = [rows_of(me)]
    for shift in range(1, n_head):
        pairs = [(i, (i + shift) % n_head) for i in range(n_head)]
        pieces.append(lax.ppermute(rows_of(lax.rem(me + shift, n_head)), "head", pairs))

    gate_rows = gates.T[:, None]
    by_head = pl.BlockSpec((tokens, HD), lambda h: (0, h))
    gate_spec = pl.BlockSpec((None, 1, tokens), lambda h: (h, 0, 0))
    params = pltpu.CompilerParams(vmem_limit_bytes=VMEM_BYTES)
    tile = SPAN * HD * HD * 2
    totals = pl.pallas_call(
        totals_kernel,
        grid=(heads,),
        in_specs=[by_head, by_head, gate_spec],
        out_specs=pl.BlockSpec((2, 1, HD, HD), lambda h: (0, h, 0, 0)),
        out_shape=jax.ShapeDtypeStruct((2, heads, HD, HD), f32),
        compiler_params=params,
        cost_estimate=pl.CostEstimate(
            flops=heads * blocks * 4 * tile, bytes_accessed=tokens * head_width * 4, transcendentals=0
        ),
        name="totals",
    )(keys, values, gate_rows)
    table = lax.all_gather(totals, "seq", axis=0)
    state = pltpu.VMEM((blocks, HD, SPAN), f32)
    readout = pl.pallas_call(
        solve_kernel,
        grid=(heads,),
        in_specs=[
            by_head, by_head, by_head, gate_spec,
            pl.BlockSpec(memory_space=pltpu.SMEM),
            pl.BlockSpec((n_seq, 2, 1, HD, HD), lambda h: (0, 0, h, 0, 0)),
        ],
        out_specs=by_head,
        out_shape=jax.ShapeDtypeStruct((tokens, head_width), bf16),
        scratch_shapes=[
            pltpu.VMEM((blocks, HD, 4 * HD), bf16),
            state, state,
            pltpu.VMEM((blocks, 3 * HD, HD), bf16),
            state, state, state,
        ],
        compiler_params=params,
        cost_estimate=pl.CostEstimate(
            flops=heads * blocks * 54 * tile, bytes_accessed=tokens * head_width * 8, transcendentals=0
        ),
        name="solve",
    )(queries, keys, values, gate_rows, ridge, table)
    width = out_weight.shape[1]
    rows = 2 * SPAN
    whole = pl.BlockSpec((head_width, width), lambda i: (0, 0))
    return pl.pallas_call(
        project_kernel,
        grid=(tokens // rows,),
        in_specs=[pl.BlockSpec((rows, head_width), lambda i: (i, 0))] + [whole] * n_head,
        out_specs=pl.BlockSpec((1, rows, width * n_head), lambda i: (0, i, 0)),
        out_shape=jax.ShapeDtypeStruct((1, tokens, width * n_head), bf16),
        compiler_params=params,
        cost_estimate=pl.CostEstimate(
            flops=2 * tokens * head_width * width * n_head,
            bytes_accessed=tokens * width * n_head * 2,
            transcendentals=0,
        ),
        name="project",
    )(readout, *pieces)


def solution(mesh):
    return jax.shard_map(
        functools.partial(shards, mesh.shape["seq"], mesh.shape["head"]),
        mesh=mesh,
        in_specs=(
            P("seq", "head"),
            P("seq", "head"),
            P("seq", "head"),
            P("seq", "head"),
            P("head"),
            P(None, "head"),
        ),
        out_specs=P("head", "seq", None),
        check_vma=False,
    )
```

```python
import functools

import jax
import jax.numpy as jnp
from jax import lax
from jax.experimental import pallas as pl
from jax.experimental.pallas import tpu as pltpu
from jax.sharding import PartitionSpec as P

HD = 128
SPAN = 128
ITERS = 8
EPS = 1e-06
f32 = jnp.float32
bf16 = jnp.bfloat16
VMEM_BYTES = 56 * 1024 * 1024


def dot(a, b):
    return jnp.dot(a, b, preferred_element_type=f32)


def two_terms(x):
    high = x.astype(bf16)
    return high, (x - high.astype(f32)).astype(bf16)


def inverse_norm(columns):
    return lax.rsqrt(jnp.sum(columns * columns, 0, keepdims=True) + EPS)


def block_sums(keys, values, gate):
    keys_t = keys.astype(f32).T
    s = inverse_norm(keys_t)
    w_value = gate * s
    w_key = w_value * s
    gram = dot(
        jnp.concatenate(two_terms(keys_t * w_key), 1), jnp.concatenate([keys, keys], 0)
    )
    moment = dot(
        jnp.concatenate(two_terms(keys_t * w_value), 1), jnp.concatenate([values, values], 0)
    )
    return gram, moment, keys_t, w_key, w_value


def gate_row(g_ref, h, rows):
    gates = g_ref[:, rows]
    return jnp.sum(
        jnp.where(lax.broadcasted_iota(jnp.int32, gates.shape, 0) == h, gates, 0.0), 0, keepdims=True
    )


def prefix_kernel(
    n_seq, k_ref, v_ref, g_ref, out_ref,
    own, mate, chip_sum, slots, give, final, mate_sems, send_sems, recv_sems, final_sems,
):
    heads = out_ref.shape[0]
    half = heads // 2
    pairs = n_seq // 2
    me = lax.axis_index("seq")
    side = lax.rem(me, 2)
    pair = me // 2
    mate_at = {"seq": me + 1 - 2 * side}
    mine = side * half
    others = (1 - side) * half

    barrier = pltpu.get_barrier_semaphore()
    pl.semaphore_signal(barrier, inc=1, device_id=mate_at, device_id_type=pl.DeviceIdType.MESH)
    for off in range(1, pairs):
        target = {"seq": lax.rem(pair + off, pairs) * 2 + side}
        pl.semaphore_signal(barrier, inc=1, device_id=target, device_id_type=pl.DeviceIdType.MESH)

    def sum_head(h):
        gram = jnp.zeros((HD, HD), f32)
        moment = jnp.zeros((HD, HD), f32)
        columns = pl.ds(pl.multiple_of(h * HD, HD), HD)
        for c in range(k_ref.shape[0] // SPAN):
            rows = pl.ds(c * SPAN, SPAN)
            block_gram, block_moment, *_ = block_sums(
                k_ref[rows, columns], v_ref[rows, columns], gate_row(g_ref, h, rows)
            )
            gram += block_gram
            moment += block_moment
        own[h, 0] = gram
        own[h, 1] = moment

    for j in range(half):
        sum_head(others + j)
    pl.semaphore_wait(barrier, pairs)
    to_mate = pltpu.make_async_remote_copy(
        src_ref=own.at[pl.ds(others, half)], dst_ref=mate,
        send_sem=mate_sems.at[0], recv_sem=mate_sems.at[1],
        device_id=mate_at, device_id_type=pl.DeviceIdType.MESH,
    )
    to_mate.start()
    for j in range(half):
        sum_head(mine + j)
    to_mate.wait()
    chip_sum[...] = own[pl.ds(mine, half)] + mate[...]

    def to_later(off):
        target = {"seq": lax.rem(pair + off, pairs) * 2 + side}
        return pltpu.make_async_remote_copy(
            src_ref=chip_sum, dst_ref=slots.at[off - 1],
            send_sem=send_sems.at[off - 1], recv_sem=recv_sems.at[off - 1],
            device_id=target, device_id_type=pl.DeviceIdType.MESH,
        )

    for off in range(1, pairs):
        @pl.when(pair + off < pairs)
        def _():
            to_later(off).start()

    give[...] = jnp.zeros(give.shape, f32)
    for off in range(1, pairs):
        @pl.when(pair >= off)
        def _():
            to_later(off).wait_recv()
            give[...] = give[...] + slots[off - 1]

    out_ref[pl.ds(mine, half)] = give[...] + side.astype(f32) * mate[...]
    give[...] = give[...] + (1 - side).astype(f32) * own[pl.ds(mine, half)]
    back = pltpu.make_async_remote_copy(
        src_ref=give, dst_ref=final,
        send_sem=final_sems.at[0], recv_sem=final_sems.at[1],
        device_id=mate_at, device_id_type=pl.DeviceIdType.MESH,
    )
    back.start()
    back.wait()
    out_ref[pl.ds(others, half)] = final[...]
    for off in range(1, pairs):
        @pl.when(pair + off < pairs)
        def _():
            to_later(off).wait_send()


def solve_kernel(
    q_ref, k_ref, v_ref, g_ref, ridge_ref, prior_ref, out_ref,
    first, second, weights, weights_value, moments, sol, res, direct,
):
    h = pl.program_id(0)
    blocks = k_ref.shape[0] // SPAN
    row = lax.broadcasted_iota(jnp.int32, (HD, HD), 0)
    col = lax.broadcasted_iota(jnp.int32, (HD, HD), 1)
    causal = row <= col
    gram = jnp.where(row == col, ridge_ref[h], 0.0) + prior_ref[0]
    moment = prior_ref[1]
    start = []
    for c in range(blocks):
        rows = pl.ds(c * SPAN, SPAN)
        block_gram, block_moment, keys_t, w_key, w_value = block_sums(
            k_ref[rows], v_ref[rows], gate_row(g_ref, h, rows)
        )
        high, low = two_terms(gram)
        keys = k_ref[rows]
        first[c, :HD] = jnp.concatenate([keys, keys], 1)
        first[c, HD:] = jnp.concatenate([high, high], 1)
        second[c] = jnp.concatenate([low, keys_t.astype(bf16)], 1)
        weights[c] = jnp.where(causal, jnp.broadcast_to(w_key, (SPAN, SPAN)).T, 0.0)
        weights_value[c] = jnp.where(causal, jnp.broadcast_to(w_value, (SPAN, SPAN)).T, 0.0)
        high, low = two_terms(moment)
        moments[c] = jnp.concatenate([high, high, low], 0)
        gram += block_gram
        moment += block_moment
        queries = q_ref[rows].astype(f32).T
        queries = queries * inverse_norm(queries)
        sol[c] = jnp.zeros((HD, SPAN), f32)
        res[c] = queries
        direct[c] = queries
        start.append(jnp.sum(queries * queries, 0, keepdims=True))

    def sweep(_, norms):
        after = []
        for c in range(blocks):
            d = direct[c]
            high, low = two_terms(d)
            both = dot(first[c], jnp.concatenate([high, low], 0))
            corr = (both[:HD] * weights[c]).astype(bf16)
            image = both[HD:] + dot(second[c], jnp.concatenate([high, corr], 0))
            now = norms[c]
            step = now / (jnp.sum(d * image, 0, keepdims=True) + EPS)
            sol[c] = sol[c] + step * d
            r = res[c] - step * image
            res[c] = r
            following = jnp.sum(r * r, 0, keepdims=True)
            direct[c] = r + following / (now + EPS) * d
            after.append(following)
        return tuple(after)

    lax.fori_loop(0, ITERS, sweep, tuple(start))
    for c in range(blocks):
        rows = pl.ds(c * SPAN, SPAN)
        keys = k_ref[rows]
        values = v_ref[rows]
        high, low = two_terms(sol[c])
        corr = dot(jnp.concatenate([keys, keys], 1), jnp.concatenate([high, low], 0))
        corr_high, corr_low = two_terms(corr * weights_value[c])
        left = jnp.concatenate([high, low, high, corr_high, corr_low], 0)
        right = jnp.concatenate([moments[c], values, values], 0)
        out_ref[rows] = lax.dot_general(
            left, right, (((0,), (0,)), ((), ())), preferred_element_type=f32
        ).astype(out_ref.dtype)


def project_kernel(r_ref, *refs):
    *pieces, out_ref = refs
    count = len(pieces)
    me = lax.axis_index("head")
    readout = r_ref[...]
    for shift, piece in enumerate(pieces):
        width = piece.shape[1]
        owner = lax.rem(me + count - shift, count)
        columns = pl.ds(pl.multiple_of(owner * width, width), width)
        out_ref[0, :, columns] = dot(readout, piece[...]).astype(out_ref.dtype)


def shards(n_seq, n_head, queries, keys, values, gates, ridge, out_weight):
    tokens, head_width = queries.shape
    heads = head_width // HD
    blocks = tokens // SPAN
    me = lax.axis_index("head")

    def rows_of(device):
        return lax.dynamic_slice_in_dim(out_weight, device * head_width, head_width, 0)

    pieces = [rows_of(me)]
    for shift in range(1, n_head):
        pairs = [(i, (i + shift) % n_head) for i in range(n_head)]
        pieces.append(lax.ppermute(rows_of(lax.rem(me + shift, n_head)), "head", pairs))

    gate_rows = gates.T
    by_head = pl.BlockSpec((tokens, HD), lambda h: (0, h))
    gate_spec = pl.BlockSpec((heads, tokens), lambda h: (0, 0))
    params = pltpu.CompilerParams(vmem_limit_bytes=VMEM_BYTES)
    tile = SPAN * HD * HD * 2
    half = heads // 2
    pairs = n_seq // 2
    part = pltpu.VMEM((half, 2, HD, HD), f32)
    in_vmem = pl.BlockSpec(memory_space=pltpu.VMEM)
    prior = pl.pallas_call(
        functools.partial(prefix_kernel, n_seq),
        in_specs=[in_vmem] * 3,
        out_specs=in_vmem,
        out_shape=jax.ShapeDtypeStruct((heads, 2, HD, HD), f32),
        scratch_shapes=[
            pltpu.VMEM((heads, 2, HD, HD), f32),
            part, part,
            pltpu.VMEM((pairs - 1, half, 2, HD, HD), f32),
            part, part,
            pltpu.SemaphoreType.DMA((2,)),
            pltpu.SemaphoreType.DMA((pairs - 1,)),
            pltpu.SemaphoreType.DMA((pairs - 1,)),
            pltpu.SemaphoreType.DMA((2,)),
        ],
        compiler_params=pltpu.CompilerParams(
            vmem_limit_bytes=VMEM_BYTES, collective_id=0, has_side_effects=True
        ),
        cost_estimate=pl.CostEstimate(
            flops=heads * blocks * 4 * tile, bytes_accessed=tokens * head_width * 4, transcendentals=0
        ),
        name="prefix",
    )(keys, values, gate_rows)
    state = pltpu.VMEM((blocks, HD, SPAN), f32)
    readout = pl.pallas_call(
        solve_kernel,
        grid=(heads,),
        in_specs=[
            by_head, by_head, by_head, gate_spec,
            pl.BlockSpec(memory_space=pltpu.SMEM),
            pl.BlockSpec((None, 2, HD, HD), lambda h: (h, 0, 0, 0)),
        ],
        out_specs=by_head,
        out_shape=jax.ShapeDtypeStruct((tokens, head_width), bf16),
        scratch_shapes=[
            pltpu.VMEM((blocks, 2 * HD, 2 * HD), bf16),
            pltpu.VMEM((blocks, HD, 2 * HD), bf16),
            state, state,
            pltpu.VMEM((blocks, 3 * HD, HD), bf16),
            state, state, state,
        ],
        compiler_params=params,
        cost_estimate=pl.CostEstimate(
            flops=heads * blocks * 54 * tile, bytes_accessed=tokens * head_width * 8, transcendentals=0
        ),
        name="solve",
    )(queries, keys, values, gate_rows, ridge, prior)
    width = out_weight.shape[1]
    rows = 2 * SPAN
    whole = pl.BlockSpec((head_width, width), lambda i: (0, 0))
    return pl.pallas_call(
        project_kernel,
        grid=(tokens // rows,),
        in_specs=[pl.BlockSpec((rows, head_width), lambda i: (i, 0))] + [whole] * n_head,
        out_specs=pl.BlockSpec((1, rows, width * n_head), lambda i: (0, i, 0)),
        out_shape=jax.ShapeDtypeStruct((1, tokens, width * n_head), bf16),
        compiler_params=params,
        cost_estimate=pl.CostEstimate(
            flops=2 * tokens * head_width * width * n_head,
            bytes_accessed=tokens * width * n_head * 2,
            transcendentals=0,
        ),
        name="project",
    )(readout, *pieces)


def solution(mesh):
    return jax.shard_map(
        functools.partial(shards, mesh.shape["seq"], mesh.shape["head"]),
        mesh=mesh,
        in_specs=(
            P("seq", "head"),
            P("seq", "head"),
            P("seq", "head"),
            P("seq", "head"),
            P("head"),
            P(None, "head"),
        ),
        out_specs=P("head", "seq", None),
        check_vma=False,
    )
```

```python
import functools

import jax
import jax.numpy as jnp
from jax import lax
from jax.experimental import pallas as pl
from jax.experimental.pallas import tpu as pltpu
from jax.sharding import PartitionSpec as P

HD = 128
SPAN = 128
ITERS = 8
EPS = 1e-06
f32 = jnp.float32
bf16 = jnp.bfloat16
VMEM_BYTES = 56 * 1024 * 1024


def dot(a, b):
    return jnp.dot(a, b, preferred_element_type=f32)


def two_terms(x):
    high = x.astype(bf16)
    return high, (x - high.astype(f32)).astype(bf16)


def inverse_norm(columns):
    return lax.rsqrt(jnp.sum(columns * columns, 0, keepdims=True) + EPS)


def block_sums(keys, values, gate):
    keys_t = keys.astype(f32).T
    s = inverse_norm(keys_t)
    w_value = gate * s
    w_key = w_value * s
    gram = dot(
        jnp.concatenate(two_terms(keys_t * w_key), 1), jnp.concatenate([keys, keys], 0)
    )
    moment = dot(
        jnp.concatenate(two_terms(keys_t * w_value), 1), jnp.concatenate([values, values], 0)
    )
    return gram, moment, keys_t, w_key, w_value


def gate_row(g_ref, h, rows):
    gates = g_ref[:, rows]
    return jnp.sum(
        jnp.where(lax.broadcasted_iota(jnp.int32, gates.shape, 0) == h, gates, 0.0), 0, keepdims=True
    )


def prefix_kernel(
    n_seq, k_ref, v_ref, g_ref, out_ref,
    own, mate, chip_sum, slots, give, final, mate_sems, send_sems, recv_sems, final_sems,
):
    heads = out_ref.shape[0]
    half = heads // 2
    pairs = n_seq // 2
    me = lax.axis_index("seq")
    side = lax.rem(me, 2)
    pair = me // 2
    mate_at = {"seq": me + 1 - 2 * side}
    mine = side * half
    others = (1 - side) * half

    barrier = pltpu.get_barrier_semaphore()
    pl.semaphore_signal(barrier, inc=1, device_id=mate_at, device_id_type=pl.DeviceIdType.MESH)
    for off in range(1, pairs):
        target = {"seq": lax.rem(pair + off, pairs) * 2 + side}
        pl.semaphore_signal(barrier, inc=1, device_id=target, device_id_type=pl.DeviceIdType.MESH)

    def sum_head(h):
        gram = jnp.zeros((HD, HD), f32)
        moment = jnp.zeros((HD, HD), f32)
        columns = pl.ds(pl.multiple_of(h * HD, HD), HD)
        for c in range(k_ref.shape[0] // SPAN):
            rows = pl.ds(c * SPAN, SPAN)
            block_gram, block_moment, *_ = block_sums(
                k_ref[rows, columns], v_ref[rows, columns], gate_row(g_ref, h, rows)
            )
            gram += block_gram
            moment += block_moment
        own[h, 0] = gram
        own[h, 1] = moment

    for j in range(half):
        sum_head(others + j)
    pl.semaphore_wait(barrier, pairs)
    to_mate = pltpu.make_async_remote_copy(
        src_ref=own.at[pl.ds(others, half)], dst_ref=mate,
        send_sem=mate_sems.at[0], recv_sem=mate_sems.at[1],
        device_id=mate_at, device_id_type=pl.DeviceIdType.MESH,
    )
    to_mate.start()
    for j in range(half):
        sum_head(mine + j)
    to_mate.wait()
    chip_sum[...] = own[pl.ds(mine, half)] + mate[...]

    def to_later(off):
        target = {"seq": lax.rem(pair + off, pairs) * 2 + side}
        return pltpu.make_async_remote_copy(
            src_ref=chip_sum, dst_ref=slots.at[off - 1],
            send_sem=send_sems.at[off - 1], recv_sem=recv_sems.at[off - 1],
            device_id=target, device_id_type=pl.DeviceIdType.MESH,
        )

    for off in range(1, pairs):
        @pl.when(pair + off < pairs)
        def _():
            to_later(off).start()

    give[...] = jnp.zeros(give.shape, f32)
    for off in range(1, pairs):
        @pl.when(pair >= off)
        def _():
            to_later(off).wait_recv()
            give[...] = give[...] + slots[off - 1]

    out_ref[pl.ds(mine, half)] = give[...] + side.astype(f32) * mate[...]
    give[...] = give[...] + (1 - side).astype(f32) * own[pl.ds(mine, half)]
    back = pltpu.make_async_remote_copy(
        src_ref=give, dst_ref=final,
        send_sem=final_sems.at[0], recv_sem=final_sems.at[1],
        device_id=mate_at, device_id_type=pl.DeviceIdType.MESH,
    )
    back.start()
    back.wait()
    out_ref[pl.ds(others, half)] = final[...]
    for off in range(1, pairs):
        @pl.when(pair + off < pairs)
        def _():
            to_later(off).wait_send()


def solve_kernel(
    q_ref, k_ref, v_ref, g_ref, ridge_ref, prior_ref, out_ref,
    first, second, weights, weights_value, moments, sol, res, direct,
    terms, corrs, images,
):
    h = pl.program_id(0)
    blocks = k_ref.shape[0] // SPAN
    row = lax.broadcasted_iota(jnp.int32, (HD, HD), 0)
    col = lax.broadcasted_iota(jnp.int32, (HD, HD), 1)
    causal = row <= col
    gram = jnp.where(row == col, ridge_ref[h], 0.0) + prior_ref[0]
    moment = prior_ref[1]
    start = []
    for c in range(blocks):
        rows = pl.ds(c * SPAN, SPAN)
        block_gram, block_moment, keys_t, w_key, w_value = block_sums(
            k_ref[rows], v_ref[rows], gate_row(g_ref, h, rows)
        )
        high, low = two_terms(gram)
        keys = k_ref[rows]
        first[c] = jnp.concatenate([keys, keys], 1)
        second[c] = jnp.concatenate([high, high, low, keys_t.astype(bf16)], 1)
        weights[c] = jnp.where(causal, jnp.broadcast_to(w_key, (SPAN, SPAN)).T, 0.0)
        weights_value[c] = jnp.where(causal, jnp.broadcast_to(w_value, (SPAN, SPAN)).T, 0.0)
        high, low = two_terms(moment)
        moments[c] = jnp.concatenate([high, high, low], 0)
        gram += block_gram
        moment += block_moment
        queries = q_ref[rows].astype(f32).T
        queries = queries * inverse_norm(queries)
        sol[c] = jnp.zeros((HD, SPAN), f32)
        res[c] = queries
        direct[c] = queries
        start.append(jnp.sum(queries * queries, 0, keepdims=True))

    def sweep(_, norms):
        after = []
        for c in range(blocks):
            high, low = two_terms(direct[c])
            terms[c, :HD] = high
            terms[c, HD:] = low
        for c in range(blocks):
            corr = dot(first[c], terms[c])
            corrs[c] = (corr * weights[c]).astype(bf16)
        for c in range(blocks):
            both = terms[c]
            images[c] = dot(second[c], jnp.concatenate([both, both[:HD], corrs[c]], 0))
        for c in range(blocks):
            d = direct[c]
            image = images[c]
            now = norms[c]
            step = now / (jnp.sum(d * image, 0, keepdims=True) + EPS)
            sol[c] = sol[c] + step * d
            r = res[c] - step * image
            res[c] = r
            following = jnp.sum(r * r, 0, keepdims=True)
            direct[c] = r + following / (now + EPS) * d
            after.append(following)
        return tuple(after)

    lax.fori_loop(0, ITERS, sweep, tuple(start))
    for c in range(blocks):
        rows = pl.ds(c * SPAN, SPAN)
        keys = k_ref[rows]
        values = v_ref[rows]
        high, low = two_terms(sol[c])
        corr = dot(jnp.concatenate([keys, keys], 1), jnp.concatenate([high, low], 0))
        corr_high, corr_low = two_terms(corr * weights_value[c])
        left = jnp.concatenate([high, low, high, corr_high, corr_low], 0)
        right = jnp.concatenate([moments[c], values, values], 0)
        out_ref[rows] = lax.dot_general(
            left, right, (((0,), (0,)), ((), ())), preferred_element_type=f32
        ).astype(out_ref.dtype)


def project_kernel(r_ref, *refs):
    *pieces, out_ref = refs
    count = len(pieces)
    me = lax.axis_index("head")
    readout = r_ref[...]
    for shift, piece in enumerate(pieces):
        width = piece.shape[1]
        owner = lax.rem(me + count - shift, count)
        columns = pl.ds(pl.multiple_of(owner * width, width), width)
        out_ref[0, :, columns] = dot(readout, piece[...]).astype(out_ref.dtype)


def shards(n_seq, n_head, queries, keys, values, gates, ridge, out_weight):
    tokens, head_width = queries.shape
    heads = head_width // HD
    blocks = tokens // SPAN
    me = lax.axis_index("head")

    def rows_of(device):
        return lax.dynamic_slice_in_dim(out_weight, device * head_width, head_width, 0)

    pieces = [rows_of(me)]
    for shift in range(1, n_head):
        pairs = [(i, (i + shift) % n_head) for i in range(n_head)]
        pieces.append(lax.ppermute(rows_of(lax.rem(me + shift, n_head)), "head", pairs))

    gate_rows = gates.T
    by_head = pl.BlockSpec((tokens, HD), lambda h: (0, h))
    gate_spec = pl.BlockSpec((heads, tokens), lambda h: (0, 0))
    params = pltpu.CompilerParams(vmem_limit_bytes=VMEM_BYTES)
    tile = SPAN * HD * HD * 2
    half = heads // 2
    pairs = n_seq // 2
    part = pltpu.VMEM((half, 2, HD, HD), f32)
    in_vmem = pl.BlockSpec(memory_space=pltpu.VMEM)
    prior = pl.pallas_call(
        functools.partial(prefix_kernel, n_seq),
        in_specs=[in_vmem] * 3,
        out_specs=in_vmem,
        out_shape=jax.ShapeDtypeStruct((heads, 2, HD, HD), f32),
        scratch_shapes=[
            pltpu.VMEM((heads, 2, HD, HD), f32),
            part, part,
            pltpu.VMEM((pairs - 1, half, 2, HD, HD), f32),
            part, part,
            pltpu.SemaphoreType.DMA((2,)),
            pltpu.SemaphoreType.DMA((pairs - 1,)),
            pltpu.SemaphoreType.DMA((pairs - 1,)),
            pltpu.SemaphoreType.DMA((2,)),
        ],
        compiler_params=pltpu.CompilerParams(
            vmem_limit_bytes=VMEM_BYTES, collective_id=0, has_side_effects=True
        ),
        cost_estimate=pl.CostEstimate(
            flops=heads * blocks * 4 * tile, bytes_accessed=tokens * head_width * 4, transcendentals=0
        ),
        name="prefix",
    )(keys, values, gate_rows)
    state = pltpu.VMEM((blocks, HD, SPAN), f32)
    readout = pl.pallas_call(
        solve_kernel,
        grid=(heads,),
        in_specs=[
            by_head, by_head, by_head, gate_spec,
            pl.BlockSpec(memory_space=pltpu.SMEM),
            pl.BlockSpec((None, 2, HD, HD), lambda h: (h, 0, 0, 0)),
        ],
        out_specs=by_head,
        out_shape=jax.ShapeDtypeStruct((tokens, head_width), bf16),
        scratch_shapes=[
            pltpu.VMEM((blocks, HD, 2 * HD), bf16),
            pltpu.VMEM((blocks, HD, 4 * HD), bf16),
            state, state,
            pltpu.VMEM((blocks, 3 * HD, HD), bf16),
            state, state, state,
            pltpu.VMEM((blocks, 2 * HD, SPAN), bf16),
            pltpu.VMEM((blocks, HD, SPAN), bf16),
            state,
        ],
        compiler_params=params,
        cost_estimate=pl.CostEstimate(
            flops=heads * blocks * 54 * tile, bytes_accessed=tokens * head_width * 8, transcendentals=0
        ),
        name="solve",
    )(queries, keys, values, gate_rows, ridge, prior)
    width = out_weight.shape[1]
    rows = 2 * SPAN
    whole = pl.BlockSpec((head_width, width), lambda i: (0, 0))
    return pl.pallas_call(
        project_kernel,
        grid=(tokens // rows,),
        in_specs=[pl.BlockSpec((rows, head_width), lambda i: (i, 0))] + [whole] * n_head,
        out_specs=pl.BlockSpec((1, rows, width * n_head), lambda i: (0, i, 0)),
        out_shape=jax.ShapeDtypeStruct((1, tokens, width * n_head), bf16),
        compiler_params=params,
        cost_estimate=pl.CostEstimate(
            flops=2 * tokens * head_width * width * n_head,
            bytes_accessed=tokens * width * n_head * 2,
            transcendentals=0,
        ),
        name="project",
    )(readout, *pieces)


def solution(mesh):
    return jax.shard_map(
        functools.partial(shards, mesh.shape["seq"], mesh.shape["head"]),
        mesh=mesh,
        in_specs=(
            P("seq", "head"),
            P("seq", "head"),
            P("seq", "head"),
            P("seq", "head"),
            P("head"),
            P(None, "head"),
        ),
        out_specs=P("head", "seq", None),
        check_vma=False,
    )
```
